128 devices in a mesh: fsdp: 32 (over z, x_lo, y), mp: 4 (over x_hi, core).
Axes of the slice: x: 4 (x_hi: 2, x_lo: 2; x = x_hi * 2 + x_lo), y: 4, z: 4, core: 2. Of those that a mesh axis runs over, the one named last changes fastest.
Arguments:
- first_moment: float32 [1, 16, 32, 128, 1024], P(None, None, 'fsdp', 'mp'), may hold values from -20 to 20
- second_moment: float32 [1, 16, 32, 128, 1024], P(None, None, 'fsdp', 'mp'), may hold values from 0.0005 to 20
- parity_groups: int32 [4, 32], replicated, may hold values from 0 to 7, as said below
Outputs:
- first_quant: bfloat16 [1, 4096, 128, 128], P(None, ('fsdp', 'mp'))
- second_quant: bfloat16 [1, 4096, 128, 128], P(None, ('fsdp', 'mp'))
- first_scale: float32 [1, 4096], P(None, ('fsdp', 'mp'))
- second_scale: float32 [1, 4096], P(None, ('fsdp', 'mp'))
- parity: float32 [128, 2, 1, 32, 128, 128], P(('fsdp', 'mp'))
The draws below stay inside these ranges and needn't reach their ends.
Inputs may be any that keep to these rules, and one draw needn't show every extreme that they name: `parity_groups`: each row is never falling along fsdp, starts at 0 and names all 8 groups; every group of a row holds 1 to 8 consecutive shards, some group holds exactly 8, and the last group holds only the last shard.
All inputs are finite; a program needn't handle non-finite values. Where the reference program divides by a largest or mean magnitude, that divisor is 1e-20 or more.
Results may differ from the reference program's by a relative error of at most 0.005.
Values may be sent and summed in bfloat16 or wider, within the bound.
A program may use at most 128 MiB of HBM per device.

```python
import jax
import jax.numpy as jnp
from jax import lax

D = 1024
LAYERS = 1
BLK = 128
PB = 32
QB = 16
NBC = 8
NBLK = 4096
SHARDS = 128
BPD = 32
MP_DEV = 4
FS_DEV = 32
GROUPS = 8


def draw_first_moment(key, part):
    base_key = jax.random.fold_in(jax.random.fold_in(key, 11), 0)
    shape = (LAYERS, QB, PB, BLK, D)
    values = jnp.clip(jax.random.normal(base_key, shape), -6.0, 6.0)
    return values.astype(jnp.float32)


def draw_second_moment(key, part):
    base_key = jax.random.fold_in(jax.random.fold_in(key, 23), 0)
    shape = (LAYERS, QB, PB, BLK, D)
    normal = jnp.clip(jax.random.normal(base_key, shape), -6.0, 6.0)
    values = 0.01 + 0.5 * normal * normal
    return values.astype(jnp.float32)


def group_row(key):
    pick_key, fill_key = jax.random.split(key)
    slots = jnp.arange(GROUPS - 1, dtype=jnp.int32)
    widest = jax.random.randint(pick_key, (), 0, GROUPS - 1, dtype=jnp.int32)
    sizes = jnp.where(slots == widest, 8, 1).astype(jnp.int32)
    extra = FS_DEV - 1 - 8 - (GROUPS - 2)

    def add_one(step, current):
        scores = jax.random.randint(jax.random.fold_in(fill_key, step), (GROUPS - 1,), 0, 1 << 20, dtype=jnp.int32)
        scores = jnp.where(current < 8, scores, -1)
        chosen = jnp.argmax(scores).astype(jnp.int32)
        return current + (slots == chosen).astype(jnp.int32)
    sizes = lax.fori_loop(0, extra, add_one, sizes)
    ends = jnp.cumsum(sizes).astype(jnp.int32)
    position = jnp.arange(FS_DEV, dtype=jnp.int32)
    labels = jnp.sum((ends[None, :] <= position[:, None]).astype(jnp.int32), axis=1)
    return labels.astype(jnp.int32)


def draw_parity_groups(key, part):
    row_keys = jax.random.split(jax.random.fold_in(key, 37), MP_DEV)
    return jax.vmap(group_row)(row_keys).astype(jnp.int32)


def setup_inputs(seed: int = 0) -> dict:
    seeds = jax.random.split(jax.random.key(seed), 4)
    return {
        "first_moment": draw_first_moment(jax.random.fold_in(seeds[3], 71), 0),
        "second_moment": draw_second_moment(jax.random.fold_in(seeds[3], 71), 0),
        "parity_groups": draw_parity_groups(jax.random.fold_in(seeds[3], 71), 0),
    }


epsilon = 1e-6


def to_blocks(values):
    split = values.reshape(LAYERS, QB, PB, BLK, NBC, BLK)
    moved = split.transpose(0, 4, 1, 2, 3, 5)
    return moved.reshape(LAYERS, NBLK, BLK, BLK)


def quantize(blocks):
    scale = jnp.max(jnp.abs(blocks), axis=(2, 3)) + epsilon
    return (blocks / scale[:, :, None, None]).astype(jnp.bfloat16), scale


def reference(first_moment, second_moment, parity_groups):
    first_quant, first_scale = quantize(to_blocks(first_moment))
    second_quant, second_scale = quantize(to_blocks(second_moment))
    shards = jnp.stack([first_quant.astype(jnp.float32), second_quant.astype(jnp.float32)])
    shards = shards.reshape(2, LAYERS, SHARDS, BPD, BLK, BLK).transpose(2, 0, 1, 3, 4, 5)
    index = jnp.arange(SHARDS, dtype=jnp.int32)
    fsdp_of = index // MP_DEV
    model_of = index % MP_DEV
    group_of = parity_groups[model_of, fsdp_of]
    before_group = parity_groups[model_of, (fsdp_of + FS_DEV - 1) % FS_DEV]
    leading = (fsdp_of == 0) | (group_of != before_group)
    member = leading[:, None] & (model_of[:, None] == model_of[None, :]) & (group_of[None, :] == before_group[:, None])
    weights = member.astype(jnp.float32)
    flat = shards.reshape(SHARDS, 2 * LAYERS * BPD * BLK * BLK)
    parity = jnp.dot(weights, flat, precision=lax.Precision.HIGHEST).reshape(shards.shape)
    return first_quant, second_quant, first_scale, second_scale, parity
```

```python
import functools

import jax
import jax.numpy as jnp
from jax import lax
from jax.experimental import pallas as pl
from jax.experimental.pallas import tpu as pltpu
from jax.sharding import PartitionSpec as P

MESH = pl.DeviceIdType.MESH
BLK = 128
FS = 32
MP = 4
N = FS * MP
ROWS = BLK // MP
COLS = 8
SETS = 16
CHUNKS = 4
epsilon = 1e-06

QUAD = ((0, 0), (0, 1), (2, 0), (2, 1))


def where_am_i():
    f = lax.axis_index("fsdp")
    m = lax.axis_index("mp")
    return f, m


def target(f, m, step, dx2, dc):
    dy = step % 4
    dx = (step // 4) % 2 + dx2
    dz = step // 8
    z = (f // 8 + dz) % 4
    x = ((m // 2) * 2 + (f // 4) % 2 + dx) % 4
    y = (f % 4 + dy) % 4
    return z * 8 + (x % 2) * 4 + y, (x // 2) * 2 + (m % 2 + dc) % 2


def source_row(f, m, step):
    dy = step % 4
    dx = (step // 4) % 2
    dz = step // 8
    z = (f // 8 + 4 - dz) % 4
    xl = ((f // 4) % 2 + 2 - dx) % 2
    y = (f % 4 + 4 - dy) % 4
    return z * 8 + xl * 4 + y


def order(j):
    return (13 * j) % 32


def kernel(
    groups, first, second,
    first_quant, second_quant, first_scale, second_scale, parity,
    x, send_q, send_p, recv_q, recv_p,
    partial, peak_send, peak_recv, scale_send, scale_recv,
    in_sem, qs_sem, qr_sem, ps_sem, pr_sem, ks_sem, kr_sem, ss_sem, sr_sem,
):
    f, m = where_am_i()
    me = f * MP + m

    barrier = pltpu.get_barrier_semaphore()

    loads = []
    for t, ref in enumerate((first, second)):
        for b in range(CHUNKS):
            w = SETS // CHUNKS
            load = pltpu.make_async_copy(
                ref.at[pl.ds(b * w, w)], x.at[t, pl.ds(b * w, w)], in_sem.at[t * CHUNKS + b]
            )
            load.start()
            loads.append(load)

    def greet(d, carry):
        other = (me + d) % N
        pl.semaphore_signal(
            barrier, inc=1, device_id=(other // MP, other % MP), device_id_type=MESH
        )
        return carry

    lax.fori_loop(1, N, greet, 0)

    for t in range(2):
        for b in range(CHUNKS):
            loads[t * CHUNKS + b].wait()
            w = SETS // CHUNKS

            def cast(q, carry):
                for c in range(COLS):
                    v = x[t, q, :, c * BLK : (c + 1) * BLK]
                    send_q[c * SETS + q, t] = v.astype(jnp.bfloat16)
                    a = jnp.abs(v)
                    a = jnp.maximum(
                        jnp.maximum(a[0:8], a[8:16]), jnp.maximum(a[16:24], a[24:32])
                    )
                    partial[t, c * SETS + q] = a
                return carry

            lax.fori_loop(b * w, (b + 1) * w, cast, 0)
        rows = jnp.max(partial[t], axis=1)
        peak_send[t : t + 1, :] = jnp.max(rows.T, axis=0, keepdims=True)

    pl.semaphore_wait(barrier, N - 1)

    for k in range(1, MP):
        pltpu.make_async_remote_copy(
            src_ref=peak_send, dst_ref=peak_recv.at[m], send_sem=ks_sem, recv_sem=kr_sem,
            device_id=(f, (m + k) % MP), device_id_type=MESH,
        ).start()

    def send(src, dst, s_sem, r_sem, step, dx2, dc):
        tf, tm = target(f, m, step, dx2, dc)
        pltpu.make_async_remote_copy(
            src_ref=src.at[tf * MP + tm], dst_ref=dst.at[f, m], send_sem=s_sem,
            recv_sem=r_sem.at[f], device_id=(tf, tm), device_id_type=MESH,
        ).start()

    def send_all(src, dst, s_sem, r_sem):
        def one(j, carry):
            for dx2, dc in QUAD:
                send(src, dst, s_sem, r_sem, order(j), dx2, dc)
            return carry

        lax.fori_loop(1, FS, one, 0)
        for dx2, dc in QUAD[1:]:
            send(src, dst, s_sem, r_sem, 0, dx2, dc)

    send_all(send_q, recv_q, qs_sem, qr_sem)
    recv_q[f, m] = send_q[me]

    peak_recv[m] = peak_send[...]
    pltpu.make_async_copy(
        peak_recv.at[pl.ds(0, MP - 1)], peak_recv.at[pl.ds(0, MP - 1)], kr_sem
    ).wait()
    scale = jnp.max(peak_recv[...], axis=0) + epsilon
    for t in range(2):
        wide = jnp.broadcast_to(scale[t : t + 1], (BLK, N)).T
        scale_send[:, t, :] = wide

    def send_scale(j, carry):
        tf = (f + order(j)) % FS
        pltpu.make_async_remote_copy(
            src_ref=scale_send.at[tf * MP + m], dst_ref=scale_recv.at[f], send_sem=ss_sem,
            recv_sem=sr_sem, device_id=(tf, m), device_id_type=MESH,
        ).start()
        return carry

    lax.fori_loop(1, FS, send_scale, 0)
    scale_recv[f] = scale_send[me]

    for row in range(MP):

        def add(i, sums):
            d = i * MP + row
            before = groups[row, jnp.maximum(i - 1, 0)]
            lead = (groups[row, i] != before).astype(jnp.float32)
            keep = 1.0 - lead
            c = d // SETS
            q = d % SETS
            out = []
            for t in range(2):
                inv = 1.0 / scale_send[d, pl.ds(t, 1), :]
                v = x[t, q, :, pl.ds(pl.multiple_of(c * BLK, BLK), BLK)]
                v = (v * inv).astype(jnp.bfloat16).astype(jnp.float32)
                send_p[d, t] = (sums[t] * lead).astype(jnp.bfloat16)
                out.append(sums[t] * keep + v)
            return tuple(out)

        zero = jnp.zeros((ROWS, BLK), jnp.float32)
        last = lax.fori_loop(0, FS, add, (zero, zero))
        for t in range(2):
            send_p[row, t] = last[t].astype(jnp.bfloat16)

    send_all(send_p, recv_p, ps_sem, pr_sem)
    recv_p[f, m] = send_p[me]

    pltpu.make_async_copy(
        scale_recv.at[pl.ds(0, FS - 1)], scale_recv.at[pl.ds(0, FS - 1)], sr_sem
    ).wait()
    eye = lax.broadcasted_iota(jnp.int32, (FS, BLK), 0) == lax.broadcasted_iota(
        jnp.int32, (FS, BLK), 1
    )
    for t, ref in enumerate((first_scale, second_scale)):
        came = scale_recv[:, t, :]
        ref[...] = jnp.sum(jnp.where(eye, came, 0.0), axis=0, keepdims=True)[:, :FS]

    quants = (first_quant, second_quant)

    def finish_q(k):
        for t in range(2):
            inv = 1.0 / scale_recv[k, pl.ds(t, 1), :]
            for r in range(MP):
                v = recv_q[k, r, t].astype(jnp.float32)
                quants[t][k, r * ROWS : (r + 1) * ROWS, :] = (v * inv).astype(jnp.bfloat16)

    def finish_p(k):
        for t in range(2):
            for r in range(MP):
                parity[t, k, r * ROWS : (r + 1) * ROWS, :] = recv_p[k, r, t].astype(jnp.float32)

    def take(buf, sem, finish):
        def one(j, carry):
            k = source_row(f, m, order(j))
            pltpu.make_async_copy(buf.at[k], buf.at[k], sem.at[k]).wait()
            finish(k)
            return carry

        lax.fori_loop(1, FS, one, 0)
        pltpu.make_async_copy(
            buf.at[f, pl.ds(0, MP - 1)], buf.at[f, pl.ds(0, MP - 1)], sem.at[f]
        ).wait()
        finish(f)

    take(recv_q, qr_sem, finish_q)
    take(recv_p, pr_sem, finish_p)

    for src, sem in ((send_q, qs_sem), (send_p, ps_sem)):
        part = src.at[pl.ds(0, N - 1)]
        pltpu.make_async_copy(part, part, sem).wait()
    part = scale_send.at[pl.ds(0, FS - 1)]
    pltpu.make_async_copy(part, part, ss_sem).wait()
    part = peak_recv.at[pl.ds(0, MP - 1)]
    pltpu.make_async_copy(part, part, ks_sem).wait()


def shards(first_moment, second_moment, parity_groups):
    hbm = pl.BlockSpec(memory_space=pltpu.HBM)
    vmem = pl.BlockSpec(memory_space=pltpu.VMEM)
    dma = pltpu.SemaphoreType.DMA
    f32, bf16 = jnp.float32, jnp.bfloat16
    fq, sq, fs, ss, par = pl.pallas_call(
        kernel,
        out_shape=(
            jax.ShapeDtypeStruct((FS, BLK, BLK), bf16),
            jax.ShapeDtypeStruct((FS, BLK, BLK), bf16),
            jax.ShapeDtypeStruct((1, FS), f32),
            jax.ShapeDtypeStruct((1, FS), f32),
            jax.ShapeDtypeStruct((2, FS, BLK, BLK), f32),
        ),
        in_specs=[pl.BlockSpec(memory_space=pltpu.SMEM), hbm, hbm],
        out_specs=(vmem, vmem, vmem, vmem, vmem),
        scratch_shapes=[
            pltpu.VMEM((2, SETS, ROWS, COLS * BLK), f32),
            pltpu.VMEM((N, 2, ROWS, BLK), bf16),
            pltpu.VMEM((N, 2, ROWS, BLK), bf16),
            pltpu.VMEM((FS, MP, 2, ROWS, BLK), bf16),
            pltpu.VMEM((FS, MP, 2, ROWS, BLK), bf16),
            pltpu.VMEM((2, N, 8, BLK), f32),
            pltpu.VMEM((2, N), f32),
            pltpu.VMEM((MP, 2, N), f32),
            pltpu.VMEM((N, 2, BLK), f32),
            pltpu.VMEM((FS, 2, BLK), f32),
            dma((2 * CHUNKS,)),
            dma, dma((FS,)),
            dma, dma((FS,)),
            dma, dma,
            dma, dma,
        ],
        compiler_params=pltpu.CompilerParams(
            collective_id=0, has_side_effects=True, vmem_limit_bytes=40 << 20
        ),
        name="relayout",
    )(
        parity_groups,
        first_moment.reshape(SETS, ROWS, COLS * BLK),
        second_moment.reshape(SETS, ROWS, COLS * BLK),
    )
    return fq[None], sq[None], fs, ss, par.reshape(1, 2, 1, FS, BLK, BLK)


def solution(mesh):
    in_specs = (P(None, None, "fsdp", "mp", None), P(None, None, "fsdp", "mp", None), P())
    out_specs = (
        P(None, ("fsdp", "mp"), None, None),
        P(None, ("fsdp", "mp"), None, None),
        P(None, ("fsdp", "mp")),
        P(None, ("fsdp", "mp")),
        P(("fsdp", "mp"), None, None, None, None, None),
    )
    return jax.shard_map(shards, mesh=mesh, in_specs=in_specs, out_specs=out_specs, check_vma=False)
```

```python
import jax
import jax.numpy as jnp
from jax import lax
from jax.experimental import pallas as pl
from jax.experimental.pallas import tpu as pltpu
from jax.sharding import PartitionSpec as P

LOGICAL = pl.DeviceIdType.LOGICAL
BLK = 128
FS = 32
MP = 4
N = FS * MP
ROWS = BLK // MP
COLS = 8
SETS = 16
CHUNKS = 4
PARTS = 8
epsilon = 1e-06

def distance(step):
    return sum(min(v, 4 - v) for v in step[:3])


STEPS = [
    (i // 32, (i // 8) % 4, (i // 2) % 4, i % 2) for i in ((n * 53) % N for n in range(1, N))
]
STEPS.sort(key=lambda step: -distance(step))


def target(f, m, step):
    dz, dx, dy, dc = step
    z = (f // 8 + dz) % 4
    x = ((m // 2) * 2 + (f // 4) % 2 + dx) % 4
    y = (f % 4 + dy) % 4
    return (z * 8 + (x % 2) * 4 + y) * MP + (x // 2) * 2 + (m % 2 + dc) % 2


def wait_all(ref, sem, count):
    part = ref.at[pl.ds(0, count)]
    pltpu.make_async_copy(part, part, sem).wait()


def kernel(
    groups_in, first, second,
    first_quant, second_quant, scales, recv_p,
    groups, x, send_q, send_p, recv_q,
    partial, peak_send, peak_recv, scale_send, scale_recv,
    in_sem, g_sem, qs_sem, qr_sem, ps_sem, pr_sem, ks_sem, kr_sem, ss_sem, sr_sem,
):
    f = lax.axis_index("fsdp")
    m = lax.axis_index("mp")
    me = f * MP + m

    barrier = pltpu.get_barrier_semaphore()

    groups_load = pltpu.make_async_copy(groups_in, groups, g_sem)
    groups_load.start()
    loads = []
    for t, ref in enumerate((first, second)):
        for b in range(CHUNKS):
            w = SETS // CHUNKS
            load = pltpu.make_async_copy(
                ref.at[pl.ds(b * w, w)], x.at[t, pl.ds(b * w, w)], in_sem.at[t * CHUNKS + b]
            )
            load.start()
            loads.append(load)

    others = [target(f, m, step) for step in STEPS]
    for other in others:
        pl.semaphore_signal(barrier, inc=1, device_id=other, device_id_type=LOGICAL)

    for t in range(2):
        for b in range(CHUNKS):
            loads[t * CHUNKS + b].wait()
            w = SETS // CHUNKS

            def cast(q, carry):
                for c in range(COLS):
                    v = x[t, q, :, c * BLK : (c + 1) * BLK]
                    send_q[c * SETS + q, t] = v.astype(jnp.bfloat16)
                    a = jnp.abs(v)
                    a = jnp.maximum(
                        jnp.maximum(a[0:8], a[8:16]), jnp.maximum(a[16:24], a[24:32])
                    )
                    partial[t, c * SETS + q] = a
                return carry

            lax.fori_loop(b * w, (b + 1) * w, cast, 0)
        rows = jnp.max(partial[t], axis=1)
        peak_send[t : t + 1, :] = jnp.max(rows.T, axis=0, keepdims=True)

    pl.semaphore_wait(barrier, N - 1)

    for k in range(1, MP):
        pltpu.make_async_remote_copy(
            src_ref=peak_send, dst_ref=peak_recv.at[m], send_sem=ks_sem, recv_sem=kr_sem,
            device_id=f * MP + (m + k) % MP, device_id_type=LOGICAL,
        ).start()

    def send_all(src, dst, s_sem, r_sem):
        for other in others:
            pltpu.make_async_remote_copy(
                src_ref=src.at[other], dst_ref=dst.at[f, m], send_sem=s_sem, recv_sem=r_sem,
                device_id=other, device_id_type=LOGICAL,
            ).start()

    send_all(send_q, recv_q, qs_sem, qr_sem)
    recv_q[f, m] = send_q[me]

    peak_recv[m] = peak_send[...]
    wait_all(peak_recv, kr_sem, MP - 1)
    scale = jnp.max(peak_recv[...], axis=0) + epsilon
    for t in range(2):
        wide = jnp.broadcast_to(scale[t : t + 1], (BLK, N)).T
        scale_send[:, t, :] = wide

    def send_scale(j, carry):
        other = (me + j * MP) % N
        pltpu.make_async_remote_copy(
            src_ref=scale_send.at[other], dst_ref=scale_recv.at[f], send_sem=ss_sem,
            recv_sem=sr_sem, device_id=other, device_id_type=LOGICAL,
        ).start()
        return carry

    lax.fori_loop(1, FS, send_scale, 0)
    scale_recv[f] = scale_send[me]

    groups_load.wait()

    for row in range(MP):

        def add(i, sums):
            d = i * MP + row
            before = groups[row, jnp.maximum(i - 1, 0)]
            lead = (groups[row, i] != before).astype(jnp.float32)
            keep = 1.0 - lead
            c = d // SETS
            q = d % SETS
            out = []
            for t in range(2):
                inv = 1.0 / scale_send[d, pl.ds(t, 1), :]
                v = x[t, q, :, pl.ds(pl.multiple_of(c * BLK, BLK), BLK)]
                v = (v * inv).astype(jnp.bfloat16).astype(jnp.float32)
                send_p[d, t] = (sums[t] * lead).astype(jnp.bfloat16)
                out.append(sums[t] * keep + v)
            return tuple(out)

        zero = jnp.zeros((ROWS, BLK), jnp.float32)
        last = lax.fori_loop(0, FS, add, (zero, zero))
        for t in range(2):
            send_p[row, t] = last[t].astype(jnp.bfloat16)

    send_all(send_p, recv_p, ps_sem, pr_sem)
    recv_p[f, m] = send_p[me]

    wait_all(scale_recv, sr_sem, FS - 1)
    eye = lax.broadcasted_iota(jnp.int32, (FS, BLK), 0) == lax.broadcasted_iota(
        jnp.int32, (FS, BLK), 1
    )
    for t in range(2):
        came = scale_recv[:, t, :]
        scales[t] = jnp.sum(jnp.where(eye, came, 0.0), axis=0, keepdims=True)[:, :FS]

    quants = (first_quant, second_quant)

    wait_all(send_q, qr_sem, N - 1)

    def finish(k, carry):
        for t in range(2):
            inv = 1.0 / scale_recv[k, pl.ds(t, 1), :]
            for r in range(MP):
                v = recv_q[k, r, t].astype(jnp.float32)
                quants[t][k, r * ROWS : (r + 1) * ROWS, :] = (v * inv).astype(jnp.bfloat16)
        return carry

    lax.fori_loop(0, FS, finish, 0)

    wait_all(send_q, qs_sem, N - 1)
    wait_all(scale_send, ss_sem, FS - 1)
    wait_all(peak_recv, ks_sem, MP - 1)
    wait_all(send_p, ps_sem, N - 1)
    wait_all(send_p, pr_sem, N - 1)


def write(q1, q2, sc, sums, first_quant, second_quant, first_scale, second_scale, parity, wide, sem, wide_sem):
    copies = [
        pltpu.make_async_copy(q1, first_quant, sem.at[0]),
        pltpu.make_async_copy(q2, second_quant, sem.at[1]),
        pltpu.make_async_copy(sc.at[0], first_scale, sem.at[2]),
        pltpu.make_async_copy(sc.at[1], second_scale, sem.at[3]),
    ]
    for copy in copies:
        copy.start()
    w = FS // PARTS
    for b in range(PARTS):

        def widen(k, carry):
            for t in range(2):
                for r in range(MP):
                    wide[t, k, r * ROWS : (r + 1) * ROWS, :] = sums[k, r, t].astype(jnp.float32)
            return carry

        lax.fori_loop(b * w, (b + 1) * w, widen, 0)
        for t in range(2):
            part = pl.ds(b * w, w)
            copy = pltpu.make_async_copy(wide.at[t, part], parity.at[t, part], wide_sem.at[t, b])
            copy.start()
            copies.append(copy)
    for copy in copies:
        copy.wait()


def shards(first_moment, second_moment, parity_groups):
    hbm = pl.BlockSpec(memory_space=pltpu.HBM)
    vmem = pl.BlockSpec(memory_space=pltpu.VMEM)
    dma = pltpu.SemaphoreType.DMA
    f32, bf16 = jnp.float32, jnp.bfloat16
    in_hbm = lambda a: pltpu.with_memory_space_constraint(a, pltpu.HBM)
    results = pl.pallas_call(
        kernel,
        out_shape=(
            jax.ShapeDtypeStruct((FS, BLK, BLK), bf16),
            jax.ShapeDtypeStruct((FS, BLK, BLK), bf16),
            jax.ShapeDtypeStruct((2, 1, FS), f32),
            jax.ShapeDtypeStruct((FS, MP, 2, ROWS, BLK), bf16),
        ),
        in_specs=[hbm, hbm, hbm],
        out_specs=(vmem, vmem, vmem, vmem),
        scratch_shapes=[
            pltpu.SMEM((MP, FS), jnp.int32),
            pltpu.VMEM((2, SETS, ROWS, COLS * BLK), f32),
            pltpu.VMEM((N, 2, ROWS, BLK), bf16),
            pltpu.VMEM((N, 2, ROWS, BLK), bf16),
            pltpu.VMEM((FS, MP, 2, ROWS, BLK), bf16),
            pltpu.VMEM((2, N, 8, BLK), f32),
            pltpu.VMEM((2, N), f32),
            pltpu.VMEM((MP, 2, N), f32),
            pltpu.VMEM((N, 2, BLK), f32),
            pltpu.VMEM((FS, 2, BLK), f32),
            dma((2 * CHUNKS,)), dma,
            dma, dma,
            dma, dma,
            dma, dma,
            dma, dma,
        ],
        compiler_params=pltpu.CompilerParams(
            collective_id=0, has_side_effects=True, vmem_limit_bytes=24 << 20
        ),
        name="relayout",
    )(
        in_hbm(parity_groups),
        in_hbm(first_moment.reshape(SETS, ROWS, COLS * BLK)),
        in_hbm(second_moment.reshape(SETS, ROWS, COLS * BLK)),
    )
    fq, sq, fs, ss, par = pl.pallas_call(
        write,
        out_shape=(
            jax.ShapeDtypeStruct((FS, BLK, BLK), bf16),
            jax.ShapeDtypeStruct((FS, BLK, BLK), bf16),
            jax.ShapeDtypeStruct((1, FS), f32),
            jax.ShapeDtypeStruct((1, FS), f32),
            jax.ShapeDtypeStruct((2, FS, BLK, BLK), f32),
        ),
        in_specs=[vmem] * 4,
        out_specs=(hbm,) * 5,
        scratch_shapes=[pltpu.VMEM((2, FS, BLK, BLK), f32), dma((4,)), dma((2, PARTS))],
        compiler_params=pltpu.CompilerParams(vmem_limit_bytes=8 << 20),
        name="write",
    )(*results)
    return fq[None], sq[None], fs, ss, par.reshape(1, 2, 1, FS, BLK, BLK)


def solution(mesh):
    in_specs = (P(None, None, "fsdp", "mp", None), P(None, None, "fsdp", "mp", None), P())
    out_specs = (
        P(None, ("fsdp", "mp"), None, None),
        P(None, ("fsdp", "mp"), None, None),
        P(None, ("fsdp", "mp")),
        P(None, ("fsdp", "mp")),
        P(("fsdp", "mp"), None, None, None, None, None),
    )
    return jax.shard_map(shards, mesh=mesh, in_specs=in_specs, out_specs=out_specs, check_vma=False)
```

```python
import jax
import jax.numpy as jnp
from jax import lax
from jax.experimental import pallas as pl
from jax.experimental.pallas import tpu as pltpu
from jax.sharding import PartitionSpec as P

LOGICAL = pl.DeviceIdType.LOGICAL
BLK = 128
FS = 32
MP = 4
N = FS * MP
ROWS = BLK // MP
COLS = 8
SETS = 16
BAND = 4
DY = (0, 1, 3, 2)
PARTS = 8
ROUNDS = 5
epsilon = 1e-06

def distance(step):
    return sum(min(v, 4 - v) for v in step[:3])


STEPS = [
    (i // 32, (i // 8) % 4, (i // 2) % 4, i % 2) for i in ((n * 53) % N for n in range(1, N))
]
STEPS.sort(key=lambda step: -distance(step))
SHELLS = [[step for step in STEPS if distance(step) == r] for r in range(7)]
NEAR = SHELLS[0] + SHELLS[1]


def target(f, m, step):
    dz, dx, dy, dc = step
    z = (f // 8 + dz) % 4
    x = ((m // 2) * 2 + (f // 4) % 2 + dx) % 4
    y = (f % 4 + dy) % 4
    return (z * 8 + (x % 2) * 4 + y) * MP + (x // 2) * 2 + (m % 2 + dc) % 2


def wait_all(ref, sem, count):
    part = ref.at[pl.ds(0, count)]
    pltpu.make_async_copy(part, part, sem).wait()


def kernel(
    groups_in, first, second,
    first_quant, second_quant, scales, recv_p,
    groups, x, send_q, send_p, recv_q,
    partial, peak_send, peak_recv, scale_send, scale_recv,
    in_sem, g_sem, qs_sem, qr_sem, ps_sem, pr_sem, ks_sem, kr_sem, ss_sem, sr_sem, round_sem,
):
    f = lax.axis_index("fsdp")
    m = lax.axis_index("mp")
    me = f * MP + m

    barrier = pltpu.get_barrier_semaphore()

    groups_load = pltpu.make_async_copy(groups_in, groups, g_sem)
    groups_load.start()
    def near_y(dy):
        return (f % 4 + dy) % 4 * BAND

    loads = {}
    for n, dy in enumerate(DY):
        rows = pl.ds(near_y(dy), BAND)
        for t, ref in enumerate((first, second)):
            loads[dy, t] = pltpu.make_async_copy(ref.at[rows], x.at[t, rows], in_sem.at[n * 2 + t])
            loads[dy, t].start()

    def tell(sem):
        for step in NEAR:
            pl.semaphore_signal(
                sem, inc=1, device_id=target(f, m, step), device_id_type=LOGICAL
            )

    tell(barrier)

    def send(src, dst, s_sem, r_sem, steps):
        for step in steps:
            other = target(f, m, step)
            pltpu.make_async_remote_copy(
                src_ref=src.at[other], dst_ref=dst.at[f, m], send_sem=s_sem, recv_sem=r_sem,
                device_id=other, device_id_type=LOGICAL,
            ).start()

    def heard(r):
        pl.semaphore_wait(barrier if r == 0 else round_sem.at[r - 1], len(NEAR))
        if r < ROUNDS:
            tell(round_sem.at[r])

    def cast(dy):
        for t in range(2):
            loads[dy, t].wait()
        base = near_y(dy)

        def one(i, carry):
            q = base + i
            for t in range(2):
                for c in range(COLS):
                    v = x[t, q, :, c * BLK : (c + 1) * BLK]
                    send_q[c * SETS + q, t] = v.astype(jnp.bfloat16)
                    a = jnp.abs(v)
                    partial[t, c * SETS + q] = jnp.maximum(
                        jnp.maximum(a[0:8], a[8:16]), jnp.maximum(a[16:24], a[24:32])
                    )
            return carry

        lax.fori_loop(0, BAND, one, 0)

    def send_q_part(radii, dys):
        steps = [step for r in radii for step in SHELLS[r] if step[2] in dys]
        send(send_q, recv_q, qs_sem, qr_sem, steps)

    cast(0)
    cast(1)
    heard(0)
    send_q_part((0, 1), (0, 1))
    cast(3)
    heard(1)
    send_q_part((2,), (0, 1))
    cast(2)
    send_q_part((1, 2), (3,))
    heard(2)
    send_q_part((2,), (2,))

    for t in range(2):
        rows = jnp.max(partial[t], axis=1)
        peak_send[t : t + 1, :] = jnp.max(rows.T, axis=0, keepdims=True)
    for k in range(1, MP):
        pltpu.make_async_remote_copy(
            src_ref=peak_send, dst_ref=peak_recv.at[m], send_sem=ks_sem, recv_sem=kr_sem,
            device_id=f * MP + (m + k) % MP, device_id_type=LOGICAL,
        ).start()

    send(send_q, recv_q, qs_sem, qr_sem, SHELLS[3])
    for r in range(3, ROUNDS + 1):
        heard(r)
        send(send_q, recv_q, qs_sem, qr_sem, SHELLS[r + 1])
    recv_q[f, m] = send_q[me]

    peak_recv[m] = peak_send[...]
    wait_all(peak_recv, kr_sem, MP - 1)
    scale = jnp.max(peak_recv[...], axis=0) + epsilon
    for t in range(2):
        wide = jnp.broadcast_to(scale[t : t + 1], (BLK, N)).T
        scale_send[:, t, :] = wide

    def send_scale(j, carry):
        other = (me + j * MP) % N
        pltpu.make_async_remote_copy(
            src_ref=scale_send.at[other], dst_ref=scale_recv.at[f], send_sem=ss_sem,
            recv_sem=sr_sem, device_id=other, device_id_type=LOGICAL,
        ).start()
        return carry

    lax.fori_loop(1, FS, send_scale, 0)
    scale_recv[f] = scale_send[me]

    groups_load.wait()

    for row in range(MP):

        def add(i, sums):
            d = i * MP + row
            before = groups[row, jnp.maximum(i - 1, 0)]
            lead = (groups[row, i] != before).astype(jnp.float32)
            keep = 1.0 - lead
            c = d // SETS
            q = d % SETS
            out = []
            for t in range(2):
                inv = 1.0 / scale_send[d, pl.ds(t, 1), :]
                v = x[t, q, :, pl.ds(pl.multiple_of(c * BLK, BLK), BLK)]
                v = (v * inv).astype(jnp.bfloat16).astype(jnp.float32)
                send_p[d, t] = (sums[t] * lead).astype(jnp.bfloat16)
                out.append(sums[t] * keep + v)
            return tuple(out)

        zero = jnp.zeros((ROWS, BLK), jnp.float32)
        last = lax.fori_loop(0, FS, add, (zero, zero))
        for t in range(2):
            send_p[row, t] = last[t].astype(jnp.bfloat16)

    send(send_p, recv_p, ps_sem, pr_sem, STEPS)
    recv_p[f, m] = send_p[me]

    wait_all(scale_recv, sr_sem, FS - 1)
    eye = lax.broadcasted_iota(jnp.int32, (FS, BLK), 0) == lax.broadcasted_iota(
        jnp.int32, (FS, BLK), 1
    )
    for t in range(2):
        came = scale_recv[:, t, :]
        scales[t] = jnp.sum(jnp.where(eye, came, 0.0), axis=0, keepdims=True)[:, :FS]

    quants = (first_quant, second_quant)

    wait_all(send_q, qr_sem, N - 1)

    def finish(k, carry):
        for t in range(2):
            inv = 1.0 / scale_recv[k, pl.ds(t, 1), :]
            for r in range(MP):
                v = recv_q[k, r, t].astype(jnp.float32)
                quants[t][k, r * ROWS : (r + 1) * ROWS, :] = (v * inv).astype(jnp.bfloat16)
        return carry

    lax.fori_loop(0, FS, finish, 0)

    wait_all(send_q, qs_sem, N - 1)
    wait_all(scale_send, ss_sem, FS - 1)
    wait_all(peak_recv, ks_sem, MP - 1)
    wait_all(send_p, ps_sem, N - 1)
    wait_all(send_p, pr_sem, N - 1)


def write(q1, q2, sc, sums, first_quant, second_quant, first_scale, second_scale, parity, wide, sem, wide_sem):
    copies = [
        pltpu.make_async_copy(q1, first_quant, sem.at[0]),
        pltpu.make_async_copy(q2, second_quant, sem.at[1]),
        pltpu.make_async_copy(sc.at[0], first_scale, sem.at[2]),
        pltpu.make_async_copy(sc.at[1], second_scale, sem.at[3]),
    ]
    for copy in copies:
        copy.start()
    w = FS // PARTS
    for b in range(PARTS):

        def widen(k, carry):
            for t in range(2):
                for r in range(MP):
                    wide[t, k, r * ROWS : (r + 1) * ROWS, :] = sums[k, r, t].astype(jnp.float32)
            return carry

        lax.fori_loop(b * w, (b + 1) * w, widen, 0)
        for t in range(2):
            part = pl.ds(b * w, w)
            copy = pltpu.make_async_copy(wide.at[t, part], parity.at[t, part], wide_sem.at[t, b])
            copy.start()
            copies.append(copy)
    for copy in copies:
        copy.wait()


def shards(first_moment, second_moment, parity_groups):
    hbm = pl.BlockSpec(memory_space=pltpu.HBM)
    vmem = pl.BlockSpec(memory_space=pltpu.VMEM)
    dma = pltpu.SemaphoreType.DMA
    f32, bf16 = jnp.float32, jnp.bfloat16
    in_hbm = lambda a: pltpu.with_memory_space_constraint(a, pltpu.HBM)
    results = pl.pallas_call(
        kernel,
        out_shape=(
            jax.ShapeDtypeStruct((FS, BLK, BLK), bf16),
            jax.ShapeDtypeStruct((FS, BLK, BLK), bf16),
            jax.ShapeDtypeStruct((2, 1, FS), f32),
            jax.ShapeDtypeStruct((FS, MP, 2, ROWS, BLK), bf16),
        ),
        in_specs=[hbm, hbm, hbm],
        out_specs=(vmem, vmem, vmem, vmem),
        scratch_shapes=[
            pltpu.SMEM((MP, FS), jnp.int32),
            pltpu.VMEM((2, SETS, ROWS, COLS * BLK), f32),
            pltpu.VMEM((N, 2, ROWS, BLK), bf16),
            pltpu.VMEM((N, 2, ROWS, BLK), bf16),
            pltpu.VMEM((FS, MP, 2, ROWS, BLK), bf16),
            pltpu.VMEM((2, N, 8, BLK), f32),
            pltpu.VMEM((2, N), f32),
            pltpu.VMEM((MP, 2, N), f32),
            pltpu.VMEM((N, 2, BLK), f32),
            pltpu.VMEM((FS, 2, BLK), f32),
            dma((2 * len(DY),)), dma,
            dma, dma,
            dma, dma,
            dma, dma,
            dma, dma,
            pltpu.SemaphoreType.REGULAR((ROUNDS,)),
        ],
        compiler_params=pltpu.CompilerParams(
            collective_id=0, has_side_effects=True, vmem_limit_bytes=24 << 20
        ),
        name="relayout",
    )(
        in_hbm(parity_groups),
        in_hbm(first_moment.reshape(SETS, ROWS, COLS * BLK)),
        in_hbm(second_moment.reshape(SETS, ROWS, COLS * BLK)),
    )
    fq, sq, fs, ss, par = pl.pallas_call(
        write,
        out_shape=(
            jax.ShapeDtypeStruct((FS, BLK, BLK), bf16),
            jax.ShapeDtypeStruct((FS, BLK, BLK), bf16),
            jax.ShapeDtypeStruct((1, FS), f32),
            jax.ShapeDtypeStruct((1, FS), f32),
            jax.ShapeDtypeStruct((2, FS, BLK, BLK), f32),
        ),
        in_specs=[vmem] * 4,
        out_specs=(hbm,) * 5,
        scratch_shapes=[pltpu.VMEM((2, FS, BLK, BLK), f32), dma((4,)), dma((2, PARTS))],
        compiler_params=pltpu.CompilerParams(vmem_limit_bytes=8 << 20),
        name="write",
    )(*results)
    return fq[None], sq[None], fs, ss, par.reshape(1, 2, 1, FS, BLK, BLK)


def solution(mesh):
    in_specs = (P(None, None, "fsdp", "mp", None), P(None, None, "fsdp", "mp", None), P())
    out_specs = (
        P(None, ("fsdp", "mp"), None, None),
        P(None, ("fsdp", "mp"), None, None),
        P(None, ("fsdp", "mp")),
        P(None, ("fsdp", "mp")),
        P(("fsdp", "mp"), None, None, None, None, None),
    )
    return jax.shard_map(shards, mesh=mesh, in_specs=in_specs, out_specs=out_specs, check_vma=False)
```

```python
import jax
import jax.numpy as jnp
from jax import lax
from jax.experimental import pallas as pl
from jax.experimental.pallas import tpu as pltpu
from jax.sharding import PartitionSpec as P

LOGICAL = pl.DeviceIdType.LOGICAL
BLK = 128
FS = 32
MP = 4
N = FS * MP
ROWS = BLK // MP
COLS = 8
SETS = 16
BAND = 4
DY = (0, 1, 3, 2)
PARTS = 8
ROUNDS = 5
epsilon = 1e-06

def distance(step):
    return sum(min(v, 4 - v) for v in step[:3])


STEPS = [
    (i // 32, (i // 8) % 4, (i // 2) % 4, i % 2) for i in ((n * 53) % N for n in range(1, N))
]
STEPS.sort(key=lambda step: -distance(step))
SHELLS = [[step for step in STEPS if distance(step) == r] for r in range(7)]
SUMS = sorted([(i // 32, (i // 8) % 4, (i // 2) % 4, i % 2) for i in ((n * 107) % N for n in range(1, N))], key=lambda step: -distance(step))
NEAR = SHELLS[0] + SHELLS[1]


def target(f, m, step):
    dz, dx, dy, dc = step
    z = (f // 8 + dz) % 4
    x = ((m // 2) * 2 + (f // 4) % 2 + dx) % 4
    y = (f % 4 + dy) % 4
    return (z * 8 + (x % 2) * 4 + y) * MP + (x // 2) * 2 + (m % 2 + dc) % 2


def wait_all(ref, sem, count):
    part = ref.at[pl.ds(0, count)]
    pltpu.make_async_copy(part, part, sem).wait()


def kernel(
    groups_in, first, second,
    first_quant, second_quant, scales, recv_p,
    groups, x, send_q, send_p, recv_q,
    partial, peak_send, peak_recv, scale_send, scale_recv,
    in_sem, g_sem, qs_sem, qr_sem, ps_sem, pr_sem, ks_sem, kr_sem, ss_sem, sr_sem, round_sem,
):
    f = lax.axis_index("fsdp")
    m = lax.axis_index("mp")
    me = f * MP + m

    barrier = pltpu.get_barrier_semaphore()

    groups_load = pltpu.make_async_copy(groups_in, groups, g_sem)
    groups_load.start()
    def near_y(dy):
        return (f % 4 + dy) % 4 * BAND

    loads = {}
    for n, dy in enumerate(DY):
        rows = pl.ds(near_y(dy), BAND)
        for t, ref in enumerate((first, second)):
            loads[dy, t] = pltpu.make_async_copy(ref.at[rows], x.at[t, rows], in_sem.at[n * 2 + t])
            loads[dy, t].start()

    def tell(sem):
        for step in NEAR:
            pl.semaphore_signal(
                sem, inc=1, device_id=target(f, m, step), device_id_type=LOGICAL
            )

    tell(barrier)

    def send(src, dst, s_sem, r_sem, steps):
        for step in steps:
            other = target(f, m, step)
            pltpu.make_async_remote_copy(
                src_ref=src.at[other], dst_ref=dst.at[f, m], send_sem=s_sem, recv_sem=r_sem,
                device_id=other, device_id_type=LOGICAL,
            ).start()

    def heard(r):
        pl.semaphore_wait(barrier if r == 0 else round_sem.at[r - 1], len(NEAR))
        if r < ROUNDS:
            tell(round_sem.at[r])

    def cast(dy):
        for t in range(2):
            loads[dy, t].wait()
        base = near_y(dy)

        def one(i, carry):
            q = base + i
            for t in range(2):
                for c in range(COLS):
                    v = x[t, q, :, c * BLK : (c + 1) * BLK]
                    send_q[c * SETS + q, t] = v.astype(jnp.bfloat16)
                    a = jnp.abs(v)
                    partial[t, c * SETS + q] = jnp.maximum(
                        jnp.maximum(a[0:8], a[8:16]), jnp.maximum(a[16:24], a[24:32])
                    )
            return carry

        lax.fori_loop(0, BAND, one, 0)

    def send_q_part(radii, dys):
        steps = [step for r in radii for step in SHELLS[r] if step[2] in dys]
        send(send_q, recv_q, qs_sem, qr_sem, steps)

    cast(0)
    cast(1)
    heard(0)
    send_q_part((0, 1), (0, 1))
    cast(3)
    heard(1)
    send_q_part((2,), (0, 1))
    cast(2)
    send_q_part((1, 2), (3,))
    heard(2)
    send_q_part((2,), (2,))

    for t in range(2):
        rows = jnp.max(partial[t], axis=1)
        peak_send[t : t + 1, :] = jnp.max(rows.T, axis=0, keepdims=True)
    for k in range(1, MP):
        pltpu.make_async_remote_copy(
            src_ref=peak_send, dst_ref=peak_recv.at[m], send_sem=ks_sem, recv_sem=kr_sem,
            device_id=f * MP + (m + k) % MP, device_id_type=LOGICAL,
        ).start()

    send(send_q, recv_q, qs_sem, qr_sem, SHELLS[3])
    for r in range(3, ROUNDS + 1):
        heard(r)
        send(send_q, recv_q, qs_sem, qr_sem, SHELLS[r + 1])
    recv_q[f, m] = send_q[me]

    peak_recv[m] = peak_send[...]
    wait_all(peak_recv, kr_sem, MP - 1)
    scale = jnp.max(peak_recv[...], axis=0) + epsilon
    for t in range(2):
        wide = jnp.broadcast_to(scale[t : t + 1], (BLK, N)).T
        scale_send[:, t, :] = wide

    def send_scale(j, carry):
        other = (me + j * MP) % N
        pltpu.make_async_remote_copy(
            src_ref=scale_send.at[other], dst_ref=scale_recv.at[f], send_sem=ss_sem,
            recv_sem=sr_sem, device_id=other, device_id_type=LOGICAL,
        ).start()
        return carry

    lax.fori_loop(1, FS, send_scale, 0)
    scale_recv[f] = scale_send[me]

    groups_load.wait()

    for row in range(MP):

        def add(i, sums):
            d = i * MP + row
            before = groups[row, jnp.maximum(i - 1, 0)]
            lead = (groups[row, i] != before).astype(jnp.float32)
            keep = 1.0 - lead
            c = d // SETS
            q = d % SETS
            out = []
            for t in range(2):
                inv = 1.0 / scale_send[d, pl.ds(t, 1), :]
                v = x[t, q, :, pl.ds(pl.multiple_of(c * BLK, BLK), BLK)]
                v = (v * inv).astype(jnp.bfloat16).astype(jnp.float32)
                send_p[d, t] = (sums[t] * lead).astype(jnp.bfloat16)
                out.append(sums[t] * keep + v)
            return tuple(out)

        zero = jnp.zeros((ROWS, BLK), jnp.float32)
        last = lax.fori_loop(0, FS, add, (zero, zero))
        for t in range(2):
            send_p[row, t] = last[t].astype(jnp.bfloat16)

    send(send_p, recv_p, ps_sem, pr_sem, SUMS)
    recv_p[f, m] = send_p[me]

    wait_all(scale_recv, sr_sem, FS - 1)
    eye = lax.broadcasted_iota(jnp.int32, (FS, BLK), 0) == lax.broadcasted_iota(
        jnp.int32, (FS, BLK), 1
    )
    for t in range(2):
        came = scale_recv[:, t, :]
        scales[t] = jnp.sum(jnp.where(eye, came, 0.0), axis=0, keepdims=True)[:, :FS]

    quants = (first_quant, second_quant)

    wait_all(send_q, qr_sem, N - 1)

    def finish(k, carry):
        for t in range(2):
            inv = 1.0 / scale_recv[k, pl.ds(t, 1), :]
            for r in range(MP):
                v = recv_q[k, r, t].astype(jnp.float32)
                quants[t][k, r * ROWS : (r + 1) * ROWS, :] = (v * inv).astype(jnp.bfloat16)
        return carry

    lax.fori_loop(0, FS, finish, 0)

    wait_all(send_q, qs_sem, N - 1)
    wait_all(scale_send, ss_sem, FS - 1)
    wait_all(peak_recv, ks_sem, MP - 1)
    wait_all(send_p, ps_sem, N - 1)
    wait_all(send_p, pr_sem, N - 1)


def write(q1, q2, sc, sums, first_quant, second_quant, first_scale, second_scale, parity, wide, sem, wide_sem):
    copies = [
        pltpu.make_async_copy(q1, first_quant, sem.at[0]),
        pltpu.make_async_copy(q2, second_quant, sem.at[1]),
        pltpu.make_async_copy(sc.at[0], first_scale, sem.at[2]),
        pltpu.make_async_copy(sc.at[1], second_scale, sem.at[3]),
    ]
    for copy in copies:
        copy.start()
    w = FS // PARTS
    for b in range(PARTS):

        def widen(k, carry):
            for t in range(2):
                for r in range(MP):
                    wide[t, k, r * ROWS : (r + 1) * ROWS, :] = sums[k, r, t].astype(jnp.float32)
            return carry

        lax.fori_loop(b * w, (b + 1) * w, widen, 0)
        for t in range(2):
            part = pl.ds(b * w, w)
            copy = pltpu.make_async_copy(wide.at[t, part], parity.at[t, part], wide_sem.at[t, b])
            copy.start()
            copies.append(copy)
    for copy in copies:
        copy.wait()


def shards(first_moment, second_moment, parity_groups):
    hbm = pl.BlockSpec(memory_space=pltpu.HBM)
    vmem = pl.BlockSpec(memory_space=pltpu.VMEM)
    dma = pltpu.SemaphoreType.DMA
    f32, bf16 = jnp.float32, jnp.bfloat16
    in_hbm = lambda a: pltpu.with_memory_space_constraint(a, pltpu.HBM)
    results = pl.pallas_call(
        kernel,
        out_shape=(
            jax.ShapeDtypeStruct((FS, BLK, BLK), bf16),
            jax.ShapeDtypeStruct((FS, BLK, BLK), bf16),
            jax.ShapeDtypeStruct((2, 1, FS), f32),
            jax.ShapeDtypeStruct((FS, MP, 2, ROWS, BLK), bf16),
        ),
        in_specs=[hbm, hbm, hbm],
        out_specs=(vmem, vmem, vmem, vmem),
        scratch_shapes=[
            pltpu.SMEM((MP, FS), jnp.int32),
            pltpu.VMEM((2, SETS, ROWS, COLS * BLK), f32),
            pltpu.VMEM((N, 2, ROWS, BLK), bf16),
            pltpu.VMEM((N, 2, ROWS, BLK), bf16),
            pltpu.VMEM((FS, MP, 2, ROWS, BLK), bf16),
            pltpu.VMEM((2, N, 8, BLK), f32),
            pltpu.VMEM((2, N), f32),
            pltpu.VMEM((MP, 2, N), f32),
            pltpu.VMEM((N, 2, BLK), f32),
            pltpu.VMEM((FS, 2, BLK), f32),
            dma((2 * len(DY),)), dma,
            dma, dma,
            dma, dma,
            dma, dma,
            dma, dma,
            pltpu.SemaphoreType.REGULAR((ROUNDS,)),
        ],
        compiler_params=pltpu.CompilerParams(
            collective_id=0, has_side_effects=True, vmem_limit_bytes=24 << 20
        ),
        name="relayout",
    )(
        in_hbm(parity_groups),
        in_hbm(first_moment.reshape(SETS, ROWS, COLS * BLK)),
        in_hbm(second_moment.reshape(SETS, ROWS, COLS * BLK)),
    )
    fq, sq, fs, ss, par = pl.pallas_call(
        write,
        out_shape=(
            jax.ShapeDtypeStruct((FS, BLK, BLK), bf16),
            jax.ShapeDtypeStruct((FS, BLK, BLK), bf16),
            jax.ShapeDtypeStruct((1, FS), f32),
            jax.ShapeDtypeStruct((1, FS), f32),
            jax.ShapeDtypeStruct((2, FS, BLK, BLK), f32),
        ),
        in_specs=[vmem] * 4,
        out_specs=(hbm,) * 5,
        scratch_shapes=[pltpu.VMEM((2, FS, BLK, BLK), f32), dma((4,)), dma((2, PARTS))],
        compiler_params=pltpu.CompilerParams(vmem_limit_bytes=8 << 20),
        name="write",
    )(*results)
    return fq[None], sq[None], fs, ss, par.reshape(1, 2, 1, FS, BLK, BLK)


def solution(mesh):
    in_specs = (P(None, None, "fsdp", "mp", None), P(None, None, "fsdp", "mp", None), P())
    out_specs = (
        P(None, ("fsdp", "mp"), None, None),
        P(None, ("fsdp", "mp"), None, None),
        P(None, ("fsdp", "mp")),
        P(None, ("fsdp", "mp")),
        P(("fsdp", "mp"), None, None, None, None, None),
    )
    return jax.shard_map(shards, mesh=mesh, in_specs=in_specs, out_specs=out_specs, check_vma=False)
```
